32 devices in a mesh: member: 2 (over x), tensor: 4 (over y, core), answer: 4 (over z).
Axes of the slice: x: 2, y: 2, z: 4, core: 2. Of those that a mesh axis runs over, the one named last changes fastest.
Arguments:
- master: float32 [5120, 13824], P('member', ('tensor', 'answer')), may hold values from -6 to 6
- left_noise: bfloat16 [256, 5120], P(('member', 'answer')), may hold values from -5 to 5
- right_noise: bfloat16 [256, 13824], P(('member', 'answer'), 'tensor'), may hold values from -5 to 5
- returns: float32 [256, 512], P('member', 'answer'), may hold values from -12 to 12
Outputs:
- new_master: float32 [5120, 13824], P('member', ('tensor', 'answer'))
- rollout: bfloat16 [5120, 13824], P(('member', 'answer'), 'tensor')
The draws below stay inside these ranges and needn't reach their ends.
All inputs are finite; a program needn't handle non-finite values.
Results may differ from the reference program's by a relative error of at most 0.01.
Values may be sent and summed in bfloat16 or wider, within the bound.
A program may use at most 64 MiB of HBM per device.

```python
import jax
import jax.numpy as jnp
from jax import lax

DMODEL = 5120
DFF = 13824
POP = 256
ANSWERS = 512


def draw_returns(key, part):
    position = jnp.arange(POP, dtype=jnp.float32) / max(POP - 1, 1)
    rising = 1.0 + 2.0 * position
    base = jax.random.normal(key, (POP, ANSWERS), jnp.float32)
    offset = 0.1
    return jnp.clip((base + offset) * rising[:, None], -12.0, 12.0)


def level_of(rng, shape, cuts, least, high):
    level, own = 1.0, jax.random.fold_in(rng, 6)
    for dim, blocks in cuts:
        draws = jnp.exp(jax.random.uniform(jax.random.fold_in(own, dim), (blocks,), jnp.float32, least / len(cuts), high / len(cuts)))
        level = level * jnp.repeat(draws, shape[dim] // blocks).reshape([-1 if axis == dim else 1 for axis in range(len(shape))])
    return level


def centred(own_key, shape, spread, bound, shards=(), kind=jnp.bfloat16):
    array = spread * jax.random.normal(own_key, shape, jnp.float32)
    if shards:
        array = array * level_of(own_key, shape, shards, -0.22, 0.18)
    return jnp.clip(array, -bound, bound).astype(kind)


def setup_inputs(seed: int = 0) -> dict:
    splits = jax.random.split(jax.random.key(seed), 5)
    return {
        "master": centred(splits[0], (DMODEL, DFF), 1.0, 6.0, ((0, 2), (1, 16)), jnp.float32),
        "left_noise": centred(splits[1], (POP, DMODEL), 1.0, 5.0, ((0, 8),)),
        "right_noise": centred(splits[2], (POP, DFF), 1.0, 5.0, ((0, 8), (1, 4))),
        "returns": draw_returns(jax.random.fold_in(splits[4], 71), 0),
    }


def reference(master, left_noise, right_noise, returns):
    scores = lax.optimization_barrier(jnp.sum(returns, axis=1))
    population = scores.shape[0]
    average = jnp.sum(scores) / population
    variance = jnp.sum(scores * scores) / population - average * average
    fitness = (scores - average) / jnp.sqrt(variance + 1e-05)
    weighted = left_noise.astype(jnp.float32) * fitness[:, None]
    update = lax.dot_general(weighted, right_noise.astype(jnp.float32), (((0,), (0,)), ((), ())), precision=lax.Precision.HIGHEST)
    new_master = master + update / jnp.sqrt(jnp.float32(population))
    return (new_master, new_master.astype(jnp.bfloat16))
```

```python
import jax
import jax.numpy as jnp
from jax import lax
from jax.experimental import pallas as pl
from jax.experimental.pallas import tpu as pltpu
from jax.sharding import PartitionSpec as P


def contract(left_tile, accum, pieces):
    right_cols, weights = pieces
    weighted = left_tile.astype(jnp.float32) * weights[:, None]
    return accum + lax.dot_general(
        weighted,
        right_cols.astype(jnp.float32),
        (((0,), (0,)), ((), ())),
        precision=lax.Precision.HIGHEST,
    )


def plain_body(master, left_noise, right_noise, returns):
    member_count = lax.axis_size("member")
    answer_count = lax.axis_size("answer")
    partial_value = jnp.sum(returns, axis=1)
    block_len = partial_value.shape[0]
    population = block_len * member_count
    scores = lax.psum(partial_value, "answer")
    score_sum, square_sum = lax.psum((jnp.sum(scores), jnp.sum(scores * scores)), "member")
    average = score_sum / population
    variance = square_sum / population - average * average
    fitness = (scores - average) / jnp.sqrt(variance + 1e-05)
    tile_rows = master.shape[0]
    local_members = left_noise.shape[0]
    restricted = lax.all_to_all(left_noise, "member", split_axis=1, concat_axis=0, tiled=True)
    gathered_rows = lax.all_gather(restricted, "answer", axis=0, tiled=True)
    width = gathered_rows.shape[1]
    left_tile = gathered_rows.reshape(answer_count, member_count, local_members, width)
    left_tile = jnp.transpose(left_tile, (1, 0, 2, 3)).reshape(
        answer_count * member_count * local_members, width
    )
    right_block = lax.all_to_all(right_noise, "answer", split_axis=1, concat_axis=0, tiled=True)
    initial = jnp.zeros((tile_rows, right_block.shape[1]), jnp.float32)
    update = contract(
        left_tile,
        initial,
        (
            lax.all_gather(right_block, "member", axis=0, tiled=True),
            lax.all_gather(fitness.astype(jnp.bfloat16), "member", axis=0, tiled=True).astype(
                jnp.float32
            ),
        ),
    )
    new_master = master + update / jnp.sqrt(jnp.float32(population))
    rollout = lax.all_to_all(
        new_master.astype(jnp.bfloat16), "answer", split_axis=0, concat_axis=1, tiled=True
    )
    return (new_master, rollout)


def exchange_kernel(members, tensors, answers, left_ref, right_ref, part_ref, l_ref, r_ref, s_ref,
                    l_send, l_recv, y_send, y_recv, c_send, c_recv, r_send, r_recv,
                    x_send, x_recv, s_send, s_recv, own_sem):
    me, te, an = lax.axis_index("member"), lax.axis_index("tensor"), lax.axis_index("answer")
    rows = left_ref.shape[0]
    tile = l_ref.shape[1]
    part = tile // tensors
    ahead = lambda i, d, n: lax.rem(i + d, n)
    behind = lambda i, d, n: lax.rem(i + n - d, n)
    slot = lambda dm, da: behind(me, dm, members) * answers + behind(an, da, answers)
    core = te + 1 - 2 * lax.rem(te, 2)
    across = lax.rem(te + tensors // 2, tensors)
    across_core = across + 1 - 2 * lax.rem(across, 2)
    steps = [(dm, da) for da in range(answers - 1, -1, -1) for dm in range(members)]
    steps = sorted(steps, key=lambda s: (s == (0, 0), s[1] == 0, s))

    barrier = pltpu.get_barrier_semaphore()
    greeted = 0
    for dm, da in steps:
        if (dm, da) != (0, 0):
            pl.semaphore_signal(barrier, inc=1,
                                device_id={"member": ahead(me, dm, members), "answer": ahead(an, da, answers)},
                                device_id_type=pl.DeviceIdType.MESH)
            greeted += 1
    for other in (core, across):
        pl.semaphore_signal(barrier, inc=1, device_id={"tensor": other}, device_id_type=pl.DeviceIdType.MESH)
        greeted += 1
    pl.semaphore_wait(barrier, greeted)

    def remote(src, dst, send, recv, where):
        copy = pltpu.make_async_remote_copy(src_ref=src, dst_ref=dst, send_sem=send, recv_sem=recv,
                                            device_id=where, device_id_type=pl.DeviceIdType.MESH)
        copy.start()
        return copy

    def l_at(s, t):
        return l_ref.at[pl.ds(pl.multiple_of(s * rows, rows), rows), pl.ds(pl.multiple_of(t * part, part), part)]

    def r_at(s):
        return r_ref.at[pl.ds(pl.multiple_of(s * rows, rows), rows), :]

    mine = slot(0, 0)
    left_copies, right_copies, part_copies, sent = {}, {}, {}, []
    own_l = pltpu.make_async_copy(
        left_ref.at[:, pl.ds(pl.multiple_of(me * tile + te * part, part), part)], l_at(mine, te), own_sem.at[0])
    own_r = pltpu.make_async_copy(right_ref.at[an], r_at(mine), own_sem.at[1])
    own_s = pltpu.make_async_copy(part_ref, s_ref.at[mine], own_sem.at[2])
    own_l.start()
    own_r.start()
    own_s.start()
    for dm, da in steps:
        if (dm, da) == (0, 0):
            continue
        to_m, to_a = ahead(me, dm, members), ahead(an, da, answers)
        where = {"member": to_m, "answer": to_a}
        left_copies[dm, da] = remote(
            left_ref.at[:, pl.ds(pl.multiple_of(to_m * tile + te * part, part), part)], l_at(mine, te),
            l_send.at[dm, da], l_recv.at[dm, da], where)
        part_copies[dm, da] = remote(part_ref, s_ref.at[mine], s_send.at[dm, da], s_recv.at[dm, da], where)
        if dm == 0:
            right_copies[da] = remote(right_ref.at[to_a], r_at(mine), r_send.at[da], r_recv.at[da], where)

    order = steps[-1:] + sorted([s for s in steps if s != (0, 0)], key=lambda s: (s[1] == 2, s[1] != 0, s))
    y_copies, c_copies, x_copies = {}, {}, {}

    def relay(dm, da):
        if (dm, da) == (0, 0):
            own_l.wait()
        else:
            left_copies[dm, da].wait_recv()
        block = l_at(slot(dm, da), te)
        y_copies[dm, da] = remote(block, block, y_send.at[dm, da], y_recv.at[dm, da], {"tensor": across})
        c_copies[0, dm, da] = remote(block, block, c_send.at[0, dm, da], c_recv.at[0, dm, da], {"tensor": core})
        if dm == 0:
            if da == 0:
                own_r.wait()
            else:
                right_copies[da].wait_recv()
            for dx in range(1, members):
                block = r_at(slot(0, da))
                x_copies[dx, da] = remote(block, block, x_send.at[dx, da], x_recv.at[dx, da],
                                          {"member": ahead(me, dx, members)})

    for dm, da in order:
        relay(dm, da)
    for dm, da in order:
        y_copies[dm, da].wait_recv()
        block = l_at(slot(dm, da), across)
        c_copies[1, dm, da] = remote(block, block, c_send.at[1, dm, da], c_recv.at[1, dm, da], {"tensor": core})
    own_s.wait()
    for copy in part_copies.values():
        copy.wait_recv()
    for copy in list(x_copies.values()) + list(c_copies.values()):
        copy.wait_recv()
    for group in (left_copies, right_copies, part_copies, y_copies, c_copies, x_copies):
        for copy in group.values():
            copy.wait_send()


def exchange(left_noise, right_blocks, partial_value, members, tensors, answers, tile):
    rows = left_noise.shape[0]
    count = members * answers
    width = right_blocks.shape[2]
    block = partial_value.shape[1]
    sems = pltpu.SemaphoreType.DMA
    pair = sems((members, answers))
    vmem = pl.BlockSpec(memory_space=pltpu.VMEM)
    return pl.pallas_call(
        lambda *refs: exchange_kernel(members, tensors, answers, *refs),
        out_shape=(
            jax.ShapeDtypeStruct((count * rows, tile), jnp.bfloat16),
            jax.ShapeDtypeStruct((count * rows, width), jnp.bfloat16),
            jax.ShapeDtypeStruct((count, 1, block), jnp.float32),
        ),
        in_specs=[vmem] * 3,
        out_specs=(vmem,) * 3,
        scratch_shapes=[
            pair, pair, pair, pair,
            sems((2, members, answers)), sems((2, members, answers)),
            sems((answers,)), sems((answers,)), pair, pair, pair, pair, sems((3,)),
        ],
        compiler_params=pltpu.CompilerParams(collective_id=0, has_side_effects=True),
        name="exchange",
    )(left_noise, right_blocks, partial_value)


def assemble_kernel(answers, own_ref, *refs):
    *far, out_ref = refs
    an = lax.axis_index("answer")
    blocks = (own_ref,) + tuple(far)
    width = own_ref.shape[1]
    for a in range(answers):
        @pl.when(an == a)
        def _(a=a):
            for j in range(answers):
                out_ref[:, j * width:(j + 1) * width] = blocks[(a - j) % answers][...]


def assemble(blocks, answers):
    rows, width = blocks[0].shape
    chunk = rows
    for size in (128, 80, 64, 40, 32, 16, 8):
        if rows % size == 0:
            chunk = size
            break
    spec = pl.BlockSpec((chunk, width), lambda i: (i, 0))
    return pl.pallas_call(
        lambda *refs: assemble_kernel(answers, *refs),
        grid=(rows // chunk,),
        out_shape=jax.ShapeDtypeStruct((rows, width * answers), blocks[0].dtype),
        in_specs=[spec] * answers,
        out_specs=pl.BlockSpec((chunk, width * answers), lambda i: (i, 0)),
        name="assemble",
    )(*blocks)


def fast_body(master, left_noise, right_noise, returns):
    members, tensors, answers = (lax.axis_size(n) for n in ("member", "tensor", "answer"))
    an = lax.axis_index("answer")
    tile, width = master.shape
    partial_value = jnp.sum(returns, axis=1)[None, :]
    right_blocks = jnp.transpose(right_noise.reshape(right_noise.shape[0], answers, width), (1, 0, 2))
    left_tile, right_block, parts = exchange(left_noise, right_blocks, partial_value, members, tensors, answers, tile)
    scores = jnp.sum(parts.reshape(members, answers, -1), axis=1).reshape(-1)
    population = scores.shape[0]
    average = jnp.sum(scores) / population
    variance = jnp.sum(scores * scores) / population - average * average
    fitness = (scores - average) / jnp.sqrt(variance + 1e-05)
    scale = fitness / jnp.sqrt(jnp.float32(population))
    weighted = (left_tile.astype(jnp.float32) * scale[:, None]).astype(jnp.bfloat16)
    update = lax.dot_general(weighted, right_block, (((0,), (0,)), ((), ())), preferred_element_type=jnp.float32)
    new_master = master + update
    rounded = new_master.astype(jnp.bfloat16)
    rows = tile // answers
    pick = lambda d: lax.dynamic_slice_in_dim(rounded, lax.rem(an + d, answers) * rows, rows, 0)
    far = {}
    for d in sorted(range(1, answers), key=lambda d: d != 2):
        far[d] = lax.ppermute(pick(d), "answer", [(i, (i + d) % answers) for i in range(answers)])
    rollout = assemble([pick(0)] + [far[d] for d in range(1, answers)], answers)
    return (new_master, rollout)


def body(master, left_noise, right_noise, returns):
    tensors = lax.axis_size("tensor")
    fits = tensors == 4 and master.shape[0] % (128 * tensors) == 0 and left_noise.shape[0] % 32 == 0
    return (fast_body if fits else plain_body)(master, left_noise, right_noise, returns)


def solution(mesh):
    return jax.shard_map(
        body,
        mesh=mesh,
        in_specs=(
            P("member", ("tensor", "answer")),
            P(("member", "answer"), None),
            P(("member", "answer"), "tensor"),
            P("member", "answer"),
        ),
        out_specs=(P("member", ("tensor", "answer")), P(("member", "answer"), "tensor")),
        check_vma=False,
    )
```
